32 devices in a mesh: dp: 2 (over x), ha: 4 (over y, core), wa: 4 (over z).
Axes of the slice: x: 2, y: 2, z: 4, core: 2. Of those that a mesh axis runs over, the one named last changes fastest.
Arguments:
- queries: bfloat16 [2, 1, 4, 4, 144, 768], P('dp', None, 'ha', 'wa'), may hold values from -5 to 5
- key_tiles: bfloat16 [2, 1, 4, 4, 144, 768], P('dp', None, 'ha', 'wa'), may hold values from -5 to 5
- value_tiles: bfloat16 [2, 1, 4, 4, 144, 768], P('dp', None, 'ha', 'wa'), may hold values from -6 to 6
- out_grad: bfloat16 [2, 1, 4, 4, 144, 1536], P('dp', None, 'ha', 'wa'), may hold values from -8 to 8
- w_out: bfloat16 [1536, 768], replicated, may hold values from -0.21875 to 0.21875
- reaches: int32 [6, 6], replicated, may hold values from 0 to 1, as said below
Outputs:
- grad_query: bfloat16 [2, 1, 4, 4, 144, 768], P('dp', None, 'ha', 'wa')
- grad_key: bfloat16 [2, 1, 4, 4, 144, 768], P('dp', None, 'ha', 'wa')
- grad_value: bfloat16 [2, 1, 4, 4, 144, 768], P('dp', None, 'ha', 'wa')
- grad_w_out: float32 [1536, 768], P(('dp', 'ha', 'wa'))
The draws below stay inside these ranges and needn't reach their ends.
Inputs may be any that keep to these rules, and one draw needn't show every extreme that they name: `reaches`: some head has every entry 1, and some other head has every entry 0.
All inputs are finite; a program needn't handle non-finite values.
Results may differ from the reference program's by a relative error of at most 0.018.
Values may be sent and summed in bfloat16 or wider, within the bound.
A program may use at most 128 MiB of HBM per device.

```python
import math
import jax
import jax.numpy as jnp
from jax import lax

D = 1536
HEADS = 6
HD = 128
NT = 1
TILE = 144
HQ = 768
B = 2
NH = 4
NW = 4


def draw_queries(key, part):
    shape_rows = (B * NT * NH * NW * TILE, HQ)
    own_key = jax.random.fold_in(key, 11)
    flat_rows = jax.random.truncated_normal(own_key, -4.0, 4.0, shape_rows, jnp.float32)
    return flat_rows.reshape(B, NT, NH, NW, TILE, HQ).astype(jnp.bfloat16)


def draw_key_tiles(key, part):
    shape_rows = (B * NT * NH * NW * TILE, HQ)
    own_key = jax.random.fold_in(key, 12)
    flat_rows = jax.random.truncated_normal(own_key, -4.0, 4.0, shape_rows, jnp.float32)
    return flat_rows.reshape(B, NT, NH, NW, TILE, HQ).astype(jnp.bfloat16)


def draw_reaches(key, part):
    first_head = jax.random.randint(jax.random.fold_in(key, 21), (), 0, HEADS)
    second_head = (first_head + 1 + jax.random.randint(jax.random.fold_in(key, 22), (), 0, HEADS - 1)) % HEADS
    random_bits = jax.random.randint(jax.random.fold_in(key, 23), (HEADS, 6), 0, 2)
    head_ids = jnp.arange(HEADS)[:, None]
    chosen = jnp.where(head_ids == first_head, 1, jnp.where(head_ids == second_head, 0, random_bits))
    return chosen.astype(jnp.int32)


def spiked(result, key, source, target, blocks, factor):
    def block_of(position):
        return (jnp.arange(result.shape[position]) // (result.shape[position] // blocks)).reshape((-1,) + (1,) * (result.ndim - 1 - position))

    one_side = jax.random.permutation(key, blocks)[block_of(target)]
    other_side = (block_of(target) + blocks // 2) % blocks
    return jnp.where((block_of(source) == one_side) | (block_of(source) == other_side), factor * result, result)


def steps_of(stream_key, shape, shards, least, top_value):
    loudness = 1.0
    for axis_at, shards_of in shards:
        heights = jax.random.uniform(jax.random.fold_in(jax.random.fold_in(stream_key, 6), axis_at), (shards_of,), jnp.float32, least / len(shards), top_value / len(shards))
        loudness = loudness * jnp.repeat(jnp.exp(heights), shape[axis_at] // shards_of).reshape((-1,) + (1,) * (len(shape) - 1 - axis_at))
    return loudness


def gaussian(key, extent, deviation, limit, shards=(), kind=jnp.bfloat16):
    result = jax.random.normal(key, extent, jnp.float32) * deviation
    if len(shards) > 0:
        result = steps_of(key, extent, shards, -0.22, 0.18) * result
    return jnp.clip(result, min=-limit, max=limit).astype(kind)


def gaussian_with(rng, extent, spread, most, cuts, heavy, dtype=jnp.bfloat16):
    result = spread * jax.random.normal(rng, extent, jnp.float32)
    if cuts:
        result = result * steps_of(rng, extent, cuts, -0.22, 0.18)
    return jnp.clip(spiked(result, jax.random.fold_in(rng, 3), *heavy), -most, most).astype(dtype)


def setup_inputs(seed: int = 0) -> dict:
    arg_keys = jax.random.split(jax.random.key(seed), 7)
    return {
        "queries": draw_queries(jax.random.fold_in(arg_keys[6], 71), 0),
        "key_tiles": draw_key_tiles(jax.random.fold_in(arg_keys[6], 71), 0),
        "value_tiles": gaussian(arg_keys[2], (B, NT, NH, NW, TILE, HQ), 1.0, 6.0, ((0, 2), (2, 4), (3, 4))),
        "out_grad": gaussian_with(arg_keys[3], (B, NT, NH, NW, TILE, D), 1.0, 8.0, ((0, 2), (2, 4), (3, 4)), (3, 5, 4, 2.0)),
        "w_out": gaussian(arg_keys[4], (D, HQ), HQ ** -0.5, 0.21875),
        "reaches": draw_reaches(jax.random.fold_in(arg_keys[6], 71), 0),
    }


def neighbours(tile_field):
    padded = jnp.pad(tile_field, ((0, 0), (1, 1), (1, 1), (0, 0), (0, 0)))
    stacked = jnp.stack([jnp.stack([padded[:, row_off:row_off + NH, col_off:col_off + NW] for col_off in range(3)], 0) for row_off in range(3)], 0)
    arranged = jnp.transpose(stacked, (3, 4, 2, 0, 1, 5, 6))
    return arranged.reshape(NH, NW, NT * 9 * TILE, tile_field.shape[-1])

def fold_back(contrib):
    channels = contrib.shape[-1]
    pieces = contrib.reshape(NH, NW, NT, 3, 3, TILE, channels)
    summed = jnp.zeros((NT, NH + 2, NW + 2, TILE, channels), jnp.float32)
    for row_off in range(3):
        for col_off in range(3):
            summed = summed.at[:, row_off:row_off + NH, col_off:col_off + NW].add(jnp.transpose(pieces[:, :, :, row_off, col_off], (2, 0, 1, 3, 4)))
    return summed[:, 1:NH + 1, 1:NW + 1]

def allowed_pairs(reach_row):
    time_ids = jnp.arange(NT)
    t_delta = time_ids[None, :] - time_ids[:, None]
    time_ok = (t_delta >= -reach_row[0]) & (t_delta <= reach_row[1])
    offsets = jnp.arange(3) - 1
    row_pos = jnp.arange(NH)[:, None] + offsets[None, :]
    row_ok = ((offsets >= -reach_row[2]) & (offsets <= reach_row[3]))[None, :] & (row_pos >= 0) & (row_pos < NH)
    col_pos = jnp.arange(NW)[:, None] + offsets[None, :]
    col_ok = ((offsets >= -reach_row[4]) & (offsets <= reach_row[5]))[None, :] & (col_pos >= 0) & (col_pos < NW)
    tile_pairs = time_ok[None, None, :, :, None, None] & row_ok[:, None, None, None, :, None] & col_ok[None, :, None, None, None, :]
    expanded = jnp.broadcast_to(tile_pairs[:, :, :, None, :, :, :, None], (NH, NW, NT, TILE, NT, 3, 3, TILE))
    return expanded.reshape(NH, NW, NT * TILE, NT * 9 * TILE)

def to_columns(tile_field):
    return jnp.transpose(tile_field, (1, 2, 0, 3, 4)).reshape(NH, NW, NT * TILE, tile_field.shape[-1])

def from_columns(column_field):
    return jnp.transpose(column_field.reshape(NH, NW, NT, TILE, column_field.shape[-1]), (2, 0, 1, 3, 4))

def sample_grads(inputs, w_out, reaches):
    query_part, key_part, value_part, grad_part = inputs
    softmax_scale = 1.0 / math.sqrt(HD)
    grad_rows = grad_part.astype(jnp.float32).reshape(-1, D)
    grad_attn = jnp.dot(grad_rows, w_out.astype(jnp.float32)).astype(jnp.bfloat16).reshape(NT, NH, NW, TILE, HQ)
    attn_list, gq_list, gk_list, gv_list = ([], [], [], [])
    for head_index in range(HEADS):
        col_start = head_index * HD
        col_stop = col_start + HD
        query_head = to_columns(query_part[..., col_start:col_stop].astype(jnp.float32))
        grad_head = to_columns(grad_attn[..., col_start:col_stop].astype(jnp.float32))
        key_near = neighbours(key_part[..., col_start:col_stop].astype(jnp.float32))
        value_near = neighbours(value_part[..., col_start:col_stop].astype(jnp.float32))
        allowed = allowed_pairs(reaches[head_index])
        scores = jnp.einsum('ijad,ijbd->ijab', query_head, key_near) * softmax_scale
        masked = jnp.where(allowed, scores, -jnp.inf)
        row_peak = lax.optimization_barrier(jnp.max(masked, axis=-1, keepdims=True))
        exp_terms = jnp.exp(masked - row_peak)
        prob_rows = exp_terms / lax.optimization_barrier(jnp.sum(exp_terms, axis=-1, keepdims=True))
        probs_wide = lax.optimization_barrier(prob_rows.astype(jnp.bfloat16)).astype(jnp.float32)
        attn_head = jnp.einsum('ijab,ijbd->ijad', probs_wide, value_near).astype(jnp.bfloat16)
        row_delta = lax.optimization_barrier(jnp.sum(grad_head * attn_head.astype(jnp.float32), axis=-1, keepdims=True))
        grad_probs = jnp.einsum('ijad,ijbd->ijab', grad_head, value_near)
        grad_scores = lax.optimization_barrier((prob_rows * (grad_probs - row_delta)).astype(jnp.bfloat16)).astype(jnp.float32)
        grad_q_head = (jnp.einsum('ijab,ijbd->ijad', grad_scores, key_near) * softmax_scale).astype(jnp.bfloat16)
        grad_k_near = jnp.einsum('ijab,ijad->ijbd', grad_scores, query_head) * softmax_scale
        grad_v_near = jnp.einsum('ijab,ijad->ijbd', probs_wide, grad_head)
        attn_list.append(from_columns(attn_head))
        gq_list.append(from_columns(grad_q_head))
        gk_list.append(fold_back(grad_k_near))
        gv_list.append(fold_back(grad_v_near))
    attended = jnp.concatenate(attn_list, axis=-1)
    grad_q = jnp.concatenate(gq_list, axis=-1)
    grad_k = jnp.concatenate(gk_list, axis=-1).astype(jnp.bfloat16)
    grad_v = jnp.concatenate(gv_list, axis=-1).astype(jnp.bfloat16)
    grad_w = jnp.dot(grad_rows.T, attended.astype(jnp.float32).reshape(-1, HQ))
    return (grad_q, grad_k, grad_v, grad_w)

def reference(queries, key_tiles, value_tiles, out_grad, w_out, reaches):

    def per_sample(inputs):
        return sample_grads(inputs, w_out, reaches)
    grad_q, grad_k, grad_v, grad_w = lax.map(per_sample, (queries, key_tiles, value_tiles, out_grad))
    return (grad_q, grad_k, grad_v, lax.optimization_barrier(jnp.sum(grad_w, axis=0)))
```

```python
import functools
import math

import jax
import jax.numpy as jnp
from jax import lax
from jax.experimental import pallas as pl
from jax.experimental.pallas import tpu as pltpu
from jax.sharding import PartitionSpec as P

HD = 128
BF = jnp.bfloat16
F32 = jnp.float32
OUTSIDE = -1e30


def dot(a, b, dims):
    return lax.dot_general(a, b, (dims, ((), ())), preferred_element_type=F32)


def kernel(
    sizes, heads, q_ref, k_ref, v_ref, og_ref, w_ref, reach_ref, gq_ref, gk_ref, gv_ref, gw_ref,
    kv, q_sl, da_sl, og_s, og_g, og_t, att, s_ref, dp_ref, p_low, ds_low,
    back_out, back_in, side_out, side_in, acc, dk_sl, dq_sl, dw_out, dw_in, dw_sl,
    w_send, w_recv, h_send, h_recv, bh_send, bh_recv, bw_send, bw_recv,
    og_send, og_recv, at_send, at_recv, dw_send, dw_recv,
):
    n_dp, n_ha, n_wa = sizes
    sent = heads - 1
    tile = q_ref.shape[0]
    model = og_ref.shape[1]
    quarter = model // 4
    block = gw_ref.shape[0]
    run = n_wa * block
    scale = 1.0 / math.sqrt(HD)
    dp, ha, wa = (lax.axis_index(a) for a in ("dp", "ha", "wa"))
    dp_hi, dp_lo = dp // 2, dp % 2
    ha_hi, ha_lo = ha // 2, ha % 2
    wide = ((wa > 0, (dp, ha, wa - 1)), (wa < n_wa - 1, (dp, ha, wa + 1)))
    high = ((ha > 0, (dp, ha - 1, wa)), (ha < n_ha - 1, (dp, ha + 1, wa)))
    group = []
    for j in range(1, 4):
        d_lo = (1 - dp_lo) if j // 2 else dp_lo
        h_lo = (1 - ha_lo) if j % 2 else ha_lo
        group.append((d_lo * 2 + h_lo, (dp_hi * 2 + d_lo, ha_hi * 2 + h_lo, wa)))
    runs = (n_dp // 2) * (n_ha // 2)
    peers = runs * n_wa
    my_peer = (dp_hi * (n_ha // 2) + ha_hi) * n_wa + wa

    def peer_at(step):
        at = lax.rem(my_peer + step, peers)
        r = at // n_wa
        return at, (
            (r // (n_ha // 2)) * 2 + dp_lo,
            (r % (n_ha // 2)) * 2 + ha_lo,
            at % n_wa,
        )

    def remote(src, dst, s, r, device):
        return pltpu.make_async_remote_copy(
            src_ref=src, dst_ref=dst, send_sem=s, recv_sem=r, device_id=device,
            device_id_type=pl.DeviceIdType.MESH,
        )

    def w_copy(d, i):
        return remote(
            kv.at[i, 4], kv.at[i, 3 + 2 * (1 - d)], w_send.at[d, i], w_recv.at[d, i], wide[d][1]
        )

    def h_copy(d, c, i):
        return remote(
            kv.at[i, 3 + c], kv.at[i, 6 * (1 - d) + c], h_send.at[d, c, i], h_recv.at[d, c, i],
            high[d][1],
        )

    def bh_copy(d, i):
        return remote(
            back_out.at[i, d], back_in.at[i, d], bh_send.at[d, i], bh_recv.at[d, i], high[d][1]
        )

    def bw_copy(d, i):
        return remote(
            side_out.at[i, d], side_in.at[i, d], bw_send.at[d, i], bw_recv.at[d, i], wide[d][1]
        )

    def og_copy(j):
        member, device = group[j - 1]
        return remote(og_s.at[member], og_g.at[j], og_send.at[j - 1], og_recv.at[j - 1], device)

    def at_copy(j, i):
        return remote(
            att.at[i, 0], att.at[i, j], at_send.at[j - 1, i], at_recv.at[j - 1, i],
            group[j - 1][1],
        )

    def dw_copy(step, i):
        at, device = peer_at(step)
        return remote(
            dw_out.at[i, at], dw_in.at[i, step - 1], dw_send.at[step - 1, i],
            dw_recv.at[step - 1, i], device,
        )

    barrier = pltpu.get_barrier_semaphore()

    def greet(device):
        pl.semaphore_signal(
            barrier, inc=1, device_id=device, device_id_type=pl.DeviceIdType.MESH
        )

    for exists, device in wide + high:
        pl.when(exists)(functools.partial(greet, device))
    for _, device in group:
        greet(device)
    for step in range(1, peers):
        greet(peer_at(step)[1])

    alone = jnp.int32(0)
    for n in reversed(range(heads)):
        reach = reach_ref[n, 2] + reach_ref[n, 3] + reach_ref[n, 4] + reach_ref[n, 5]
        alone = jnp.where(reach == 0, n, alone)

    def pick(i, read):
        if i < sent:
            return jnp.where(alone <= i, read(i + 1), read(i))
        value = read(0)
        for n in range(1, heads):
            value = jnp.where(alone == n, read(n), value)
        return value

    def place(n, read):
        value = read(sent)
        if n < sent:
            value = jnp.where(alone > n, read(n), value)
        if n > 0:
            value = jnp.where(alone < n, read(n - 1), value)
        return value

    def columns(ref):
        return lambda n: ref[:, n * HD : (n + 1) * HD]

    for i in range(sent):
        kv[i, 4, :, :HD] = pick(i, columns(k_ref))
        kv[i, 4, :, HD:] = pick(i, columns(v_ref))
    for m in range(4):
        for r in range(runs):
            first = (r // (n_ha // 2) * 2 + m // 2) * n_ha + (r % (n_ha // 2)) * 2 + m % 2
            og_s[m, :, r * run : (r + 1) * run] = og_ref[:, first * run : (first + 1) * run]

    for d in range(2):
        @pl.when(jnp.logical_not(wide[d][0]))
        def _():
            for i in range(sent):
                kv[i, 3 + 2 * d] = jnp.zeros((tile, 2 * HD), BF)
                side_in[i, 1 - d] = jnp.zeros((tile, 2 * HD), BF)

        @pl.when(jnp.logical_not(high[d][0]))
        def _():
            for i in range(sent):
                kv[i, 6 * d : 6 * d + 3] = jnp.zeros((3, tile, 2 * HD), BF)
                back_in[i, 1 - d] = jnp.zeros((3, tile, 2 * HD), BF)

    waits = 3 + peers - 1
    for exists, _ in wide + high:
        waits = waits + jnp.where(exists, 1, 0)
    pl.semaphore_wait(barrier, waits)

    for i in range(sent):
        for d in range(2):
            @pl.when(wide[d][0])
            def _():
                w_copy(d, i).start()

            @pl.when(high[d][0])
            def _():
                h_copy(d, 1, i).start()
    for j in range(1, 4):
        og_copy(j).start()

    grad_attn = dot(og_ref[...], w_ref[...], ((1,), (0,))).astype(BF)
    for i in range(heads):
        q_sl[i] = pick(i, columns(q_ref))
        da_sl[i] = pick(i, columns(grad_attn))

    def attend(i, q, da, k, v, keys, bias):
        def rows(c):
            return slice(c * 16, (c + 1) * 16)

        s_ref[:, :keys] = dot(q, k, ((1,), (1,)))
        dp_ref[:, :keys] = dot(da, v, ((1,), (1,)))
        for c in range(tile // 16):
            s = s_ref[rows(c), :keys] * scale
            if bias is not None:
                s = s + bias
            e = jnp.exp(s - jnp.max(s, axis=1, keepdims=True))
            p = e * (1.0 / jnp.sum(e, axis=1, keepdims=True))
            s_ref[rows(c), :keys] = p
            p_low[rows(c), :keys] = p.astype(BF)
        attended = dot(p_low[:, :keys], v, ((1,), (0,))).astype(BF)
        att[i, 0] = attended
        delta = jnp.sum(da.astype(F32) * attended.astype(F32), axis=1, keepdims=True)
        for c in range(tile // 16):
            ds = s_ref[rows(c), :keys] * (dp_ref[rows(c), :keys] - delta[rows(c)])
            ds_low[rows(c), :keys] = ds.astype(BF)
        dq_sl[i] = (dot(ds_low[:, :keys], k, ((1,), (0,))) * scale).astype(BF)
        dk = dot(ds_low[:, :keys], q, ((0,), (0,))) * scale
        dv = dot(p_low[:, :keys], da, ((0,), (0,)))
        return dk, dv

    dk, dv = attend(
        sent, q_sl[sent], da_sl[sent], pick(sent, columns(k_ref)), pick(sent, columns(v_ref)), tile, None
    )
    dk_sl[sent, :, :HD] = dk.astype(BF)
    dk_sl[sent, :, HD:] = dv.astype(BF)
    for j in range(1, 4):
        at_copy(j, sent).start()

    def relay(i):
        for d in range(2):
            @pl.when(wide[1 - d][0])
            def _():
                w_copy(d, i).wait_recv()
        for d in range(2):
            @pl.when(high[d][0])
            def _():
                h_copy(d, 0, i).start()
                h_copy(d, 2, i).start()

    def fold_high(i):
        for d in range(2):
            @pl.when(high[1 - d][0])
            def _():
                bh_copy(d, i).wait_recv()
        for d in range(2):
            c = 2 * d
            side_out[i, d] = (
                acc[i, c] + back_in[i, 0, c].astype(F32) + back_in[i, 1, c].astype(F32)
            ).astype(BF)
        acc[i, 1] = acc[i, 1] + back_in[i, 0, 1].astype(F32) + back_in[i, 1, 1].astype(F32)
        for d in range(2):
            @pl.when(wide[d][0])
            def _():
                bw_copy(d, i).start()

    def fold_wide(i):
        for d in range(2):
            @pl.when(wide[1 - d][0])
            def _():
                bw_copy(d, i).wait_recv()
        dk_sl[i] = (
            acc[i, 1] + side_in[i, 0].astype(F32) + side_in[i, 1].astype(F32)
        ).astype(BF)

    def project(i):
        for j in range(1, 4):
            at_copy(j, i).wait_recv()
        part = dot(og_t[...], att[i].reshape(4 * tile, HD), ((1,), (0,)))
        for b in range(peers):
            dw_out[i, b] = part[b * block : (b + 1) * block].astype(BF)
        for b in range(1, peers):
            dw_copy(b, i).start()

    def window(i):
        def reach(c):
            return jnp.where(alone <= i, reach_ref[i + 1, c], reach_ref[i, c])

        tiles = lax.broadcasted_iota(jnp.int32, (1, 9 * tile), 1)
        bias = jnp.zeros((1, 9 * tile), F32)
        before = (jnp.where((ha > 0) & (reach(2) > 0), 1, 0), 1,
                  jnp.where((ha < n_ha - 1) & (reach(3) > 0), 1, 0))
        beside = (jnp.where((wa > 0) & (reach(4) > 0), 1, 0), 1,
                  jnp.where((wa < n_wa - 1) & (reach(5) > 0), 1, 0))
        for t in range(9):
            open_ = jnp.where(before[t // 3] * beside[t % 3] > 0, 0.0, OUTSIDE)
            inside = (tiles >= t * tile) & (tiles < (t + 1) * tile)
            bias = jnp.where(inside, open_, bias)
        return bias

    relay(0)
    relay(1)
    for j in range(1, 4):
        og_copy(j).wait_recv()
    og_g[0] = og_s[dp_lo * 2 + ha_lo]
    og_t[...] = og_g[...].reshape(4 * tile, quarter).T
    project(sent)

    def step(i, carry):
        pl.when(i + 2 < sent)(lambda: relay(i + 2))
        for d in range(2):
            @pl.when(high[1 - d][0])
            def _():
                for c in range(3):
                    h_copy(d, c, i).wait_recv()
        near = kv[i].reshape(9 * tile, 2 * HD)
        dk, dv = attend(
            i, q_sl[i], da_sl[i], near[:, :HD], near[:, HD:], 9 * tile, window(i)
        )
        for j in range(1, 4):
            at_copy(j, i).start()
        dk = dk.reshape(3, 3, tile, HD)
        dv = dv.reshape(3, 3, tile, HD)
        for d in range(2):
            back_out[i, d, :, :, :HD] = dk[2 * d].astype(BF)
            back_out[i, d, :, :, HD:] = dv[2 * d].astype(BF)

            @pl.when(high[d][0])
            def _():
                bh_copy(d, i).start()
        acc[i, :, :, :HD] = dk[1]
        acc[i, :, :, HD:] = dv[1]

        @pl.when(i >= 1)
        def _():
            project(i - 1)
            fold_high(i - 1)
        pl.when(i >= 2)(lambda: fold_wide(i - 2))
        return carry

    lax.fori_loop(0, sent, step, 0)
    project(sent - 1)
    fold_high(sent - 1)
    if sent > 1:
        fold_wide(sent - 2)

    for n in range(heads):
        gq_ref[:, n * HD : (n + 1) * HD] = place(n, lambda i: dq_sl[i])

    def gather_w(i, carry):
        total = dw_out[i, my_peer].astype(F32)
        for b in range(1, peers):
            dw_copy(b, i).wait_recv()
            total = total + dw_in[i, b - 1].astype(F32)
        dw_sl[i] = total
        return carry

    lax.fori_loop(0, heads, gather_w, 0)
    fold_wide(sent - 1)
    for n in range(heads):
        at = slice(n * HD, (n + 1) * HD)
        gk_ref[:, at] = place(n, lambda i: dk_sl[i, :, :HD])
        gv_ref[:, at] = place(n, lambda i: dk_sl[i, :, HD:])
        gw_ref[:, at] = place(n, lambda i: dw_sl[i])

    def drain(i, carry):
        for d in range(2):
            @pl.when(wide[d][0])
            def _():
                w_copy(d, i).wait_send()
                bw_copy(d, i).wait_send()

            @pl.when(high[d][0])
            def _():
                for c in range(3):
                    h_copy(d, c, i).wait_send()
                bh_copy(d, i).wait_send()
        return carry

    lax.fori_loop(0, sent, drain, 0)

    def drain_w(i, carry):
        for j in range(1, 4):
            at_copy(j, i).wait_send()
        for b in range(1, peers):
            dw_copy(b, i).wait_send()
        return carry

    lax.fori_loop(0, heads, drain_w, 0)
    for j in range(1, 4):
        og_copy(j).wait_send()


def shards(sizes, queries, key_tiles, value_tiles, out_grad, w_out, reaches):
    tile, width = queries.shape[4:]
    model = out_grad.shape[5]
    heads = width // HD
    sent = heads - 1
    devices = sizes[0] * sizes[1] * sizes[2]
    block = model // devices
    peers = devices // 4
    rows = [a.reshape(a.shape[-2:]) for a in (queries, key_tiles, value_tiles, out_grad)]
    sem = pltpu.SemaphoreType.DMA
    vmem = pl.BlockSpec(memory_space=pltpu.VMEM)
    grads = jax.ShapeDtypeStruct((tile, width), BF)
    out = pl.pallas_call(
        functools.partial(kernel, sizes, heads),
        out_shape=(grads, grads, grads, jax.ShapeDtypeStruct((block, width), F32)),
        in_specs=[vmem] * 5 + [pl.BlockSpec(memory_space=pltpu.SMEM)],
        out_specs=(vmem,) * 4,
        scratch_shapes=[
            pltpu.VMEM((sent, 9, tile, 2 * HD), BF),
            pltpu.VMEM((heads, tile, HD), BF),
            pltpu.VMEM((heads, tile, HD), BF),
            pltpu.VMEM((4, tile, model // 4), BF),
            pltpu.VMEM((4, tile, model // 4), BF),
            pltpu.VMEM((model // 4, 4 * tile), BF),
            pltpu.VMEM((heads, 4, tile, HD), BF),
            pltpu.VMEM((tile, 9 * tile), F32),
            pltpu.VMEM((tile, 9 * tile), F32),
            pltpu.VMEM((tile, 9 * tile), BF),
            pltpu.VMEM((tile, 9 * tile), BF),
            pltpu.VMEM((sent, 2, 3, tile, 2 * HD), BF),
            pltpu.VMEM((sent, 2, 3, tile, 2 * HD), BF),
            pltpu.VMEM((sent, 2, tile, 2 * HD), BF),
            pltpu.VMEM((sent, 2, tile, 2 * HD), BF),
            pltpu.VMEM((sent, 3, tile, 2 * HD), F32),
            pltpu.VMEM((heads, tile, 2 * HD), BF),
            pltpu.VMEM((heads, tile, HD), BF),
            pltpu.VMEM((heads, peers, block, HD), BF),
            pltpu.VMEM((heads, peers - 1, block, HD), BF),
            pltpu.VMEM((heads, block, HD), F32),
            sem((2, sent)), sem((2, sent)), sem((2, 3, sent)), sem((2, 3, sent)),
            sem((2, sent)), sem((2, sent)), sem((2, sent)), sem((2, sent)),
            sem((3,)), sem((3,)), sem((3, heads)), sem((3, heads)),
            sem((peers - 1, heads)), sem((peers - 1, heads)),
        ],
        compiler_params=pltpu.CompilerParams(
            collective_id=0, has_side_effects=True, vmem_limit_bytes=60 * 1024 * 1024
        ),
    )(*rows, w_out, reaches)
    return tuple(o.reshape(queries.shape) for o in out[:3]) + (out[3],)


def solution(mesh):
    tiles = P("dp", None, "ha", "wa", None, None)
    sizes = tuple(mesh.shape[a] for a in ("dp", "ha", "wa"))
    return jax.shard_map(
        functools.partial(shards, sizes),
        mesh=mesh,
        in_specs=(tiles, tiles, tiles, tiles, P(), P()),
        out_specs=(tiles, tiles, tiles, P(("dp", "ha", "wa"), None)),
        check_vma=False,
    )
```

```python
import functools
import math

import jax
import jax.numpy as jnp
from jax import lax
from jax.experimental import pallas as pl
from jax.experimental.pallas import tpu as pltpu
from jax.sharding import PartitionSpec as P

HD = 128
BF = jnp.bfloat16
F32 = jnp.float32
OUTSIDE = -1e30


def dot(a, b, dims):
    return lax.dot_general(a, b, (dims, ((), ())), preferred_element_type=F32)


def lone_head(heads, reach_ref):
    alone = jnp.int32(0)
    for n in reversed(range(heads)):
        reach = reach_ref[n, 2] + reach_ref[n, 3] + reach_ref[n, 4] + reach_ref[n, 5]
        alone = jnp.where(reach == 0, n, alone)
    return alone


def kernel(
    sizes, heads, q_ref, k_ref, v_ref, og_any, w_any, reach_ref, dq_sl, dk_sl, dw_sl,
    kv, q_sl, da_sl, og_s, og_g, og_t, att, s_ref, dp_ref, p_low, ds_low,
    back_out, back_in, side_out, side_in, acc, dw_out, dw_in, og_ref, w_ref, in_sem,
    w_send, w_recv, h_send, h_recv, bh_send, bh_recv, bw_send, bw_recv,
    og_send, og_recv, at_send, at_recv, dw_send, dw_recv,
):
    n_dp, n_ha, n_wa = sizes
    sent = heads - 1
    tile = q_ref.shape[0]
    model = og_ref.shape[1]
    quarter = model // 4
    block = dw_sl.shape[1]
    run = n_wa * block
    scale = 1.0 / math.sqrt(HD)
    dp, ha, wa = (lax.axis_index(a) for a in ("dp", "ha", "wa"))
    dp_hi, dp_lo = dp // 2, dp % 2
    ha_hi, ha_lo = ha // 2, ha % 2
    wide = ((wa > 0, (dp, ha, wa - 1)), (wa < n_wa - 1, (dp, ha, wa + 1)))
    high = ((ha > 0, (dp, ha - 1, wa)), (ha < n_ha - 1, (dp, ha + 1, wa)))
    group = []
    for j in range(1, 4):
        d_lo = (1 - dp_lo) if j // 2 else dp_lo
        h_lo = (1 - ha_lo) if j % 2 else ha_lo
        group.append((d_lo * 2 + h_lo, (dp_hi * 2 + d_lo, ha_hi * 2 + h_lo, wa)))
    runs = (n_dp // 2) * (n_ha // 2)
    peers = runs * n_wa
    my_peer = (dp_hi * (n_ha // 2) + ha_hi) * n_wa + wa

    def peer_at(step):
        at = lax.rem(my_peer + step, peers)
        r = at // n_wa
        return at, (
            (r // (n_ha // 2)) * 2 + dp_lo,
            (r % (n_ha // 2)) * 2 + ha_lo,
            at % n_wa,
        )

    def remote(src, dst, s, r, device):
        return pltpu.make_async_remote_copy(
            src_ref=src, dst_ref=dst, send_sem=s, recv_sem=r, device_id=device,
            device_id_type=pl.DeviceIdType.MESH,
        )

    def w_copy(d, i):
        return remote(
            kv.at[i, 4], kv.at[i, 3 + 2 * (1 - d)], w_send.at[d, i], w_recv.at[d, i], wide[d][1]
        )

    def h_copy(d, c, i):
        return remote(
            kv.at[i, 3 + c], kv.at[i, 6 * (1 - d) + c], h_send.at[d, c, i], h_recv.at[d, c, i],
            high[d][1],
        )

    def bh_copy(d, i):
        return remote(
            back_out.at[i, d], back_in.at[i, d], bh_send.at[d, i], bh_recv.at[d, i], high[d][1]
        )

    def bw_copy(d, i):
        return remote(
            side_out.at[i, d], side_in.at[i, d], bw_send.at[d, i], bw_recv.at[d, i], wide[d][1]
        )

    def og_copy(j):
        member, device = group[j - 1]
        return remote(og_s.at[member], og_g.at[j], og_send.at[j - 1], og_recv.at[j - 1], device)

    def at_copy(j, i):
        return remote(
            att.at[i, 0], att.at[i, j], at_send.at[j - 1, i], at_recv.at[j - 1, i],
            group[j - 1][1],
        )

    def dw_copy(step, i):
        at, device = peer_at(step)
        return remote(
            dw_out.at[i, at], dw_in.at[i, step - 1], dw_send.at[step - 1, i],
            dw_recv.at[step - 1, i], device,
        )

    og_in = pltpu.make_async_copy(og_any, og_ref, in_sem.at[0])
    w_in = pltpu.make_async_copy(w_any, w_ref, in_sem.at[1])
    og_in.start()
    w_in.start()
    barrier = pltpu.get_barrier_semaphore()

    def greet(device):
        pl.semaphore_signal(
            barrier, inc=1, device_id=device, device_id_type=pl.DeviceIdType.MESH
        )

    for exists, device in wide + high:
        pl.when(exists)(functools.partial(greet, device))
    for _, device in group:
        greet(device)
    for step in range(1, peers):
        greet(peer_at(step)[1])

    alone = lone_head(heads, reach_ref)

    def pick(i, read):
        if i < sent:
            return jnp.where(alone <= i, read(i + 1), read(i))
        value = read(0)
        for n in range(1, heads):
            value = jnp.where(alone == n, read(n), value)
        return value

    def columns(ref):
        return lambda n: ref[:, n * HD : (n + 1) * HD]

    for i in range(sent):
        kv[i, 4, :, :HD] = pick(i, columns(k_ref))
        kv[i, 4, :, HD:] = pick(i, columns(v_ref))
    for d in range(2):
        @pl.when(jnp.logical_not(wide[d][0]))
        def _():
            for i in range(sent):
                kv[i, 3 + 2 * d] = jnp.zeros((tile, 2 * HD), BF)
                side_in[i, 1 - d] = jnp.zeros((tile, 2 * HD), BF)

        @pl.when(jnp.logical_not(high[d][0]))
        def _():
            for i in range(sent):
                kv[i, 6 * d : 6 * d + 3] = jnp.zeros((3, tile, 2 * HD), BF)
                back_in[i, 1 - d] = jnp.zeros((3, tile, 2 * HD), BF)

    waits = 3 + peers - 1
    for exists, _ in wide + high:
        waits = waits + jnp.where(exists, 1, 0)
    pl.semaphore_wait(barrier, waits)

    for i in range(sent):
        for d in range(2):
            @pl.when(wide[d][0])
            def _():
                w_copy(d, i).start()

            @pl.when(high[d][0])
            def _():
                h_copy(d, 1, i).start()
    og_in.wait()
    for m in range(4):
        for r in range(runs):
            first = (r // (n_ha // 2) * 2 + m // 2) * n_ha + (r % (n_ha // 2)) * 2 + m % 2
            og_s[m, :, r * run : (r + 1) * run] = og_ref[:, first * run : (first + 1) * run]
    for j in range(1, 4):
        og_copy(j).start()
    w_in.wait()

    grad_attn = dot(og_ref[...], w_ref[...], ((1,), (0,))).astype(BF)
    for i in range(heads):
        q_sl[i] = pick(i, columns(q_ref))
        da_sl[i] = pick(i, columns(grad_attn))

    def attend(i, q, da, k, v, keys, bias):
        def rows(c):
            return slice(c * 16, (c + 1) * 16)

        s_ref[:, :keys] = dot(q, k, ((1,), (1,)))
        dp_ref[:, :keys] = dot(da, v, ((1,), (1,)))
        for c in range(tile // 16):
            s = s_ref[rows(c), :keys] * scale
            if bias is not None:
                s = s + bias
            e = jnp.exp(s - jnp.max(s, axis=1, keepdims=True))
            p = e * (1.0 / jnp.sum(e, axis=1, keepdims=True))
            s_ref[rows(c), :keys] = p
            p_low[rows(c), :keys] = p.astype(BF)
        attended = dot(p_low[:, :keys], v, ((1,), (0,))).astype(BF)
        att[i, 0] = attended
        delta = jnp.sum(da.astype(F32) * attended.astype(F32), axis=1, keepdims=True)
        for c in range(tile // 16):
            ds = s_ref[rows(c), :keys] * (dp_ref[rows(c), :keys] - delta[rows(c)])
            ds_low[rows(c), :keys] = ds.astype(BF)
        dq_sl[i] = (dot(ds_low[:, :keys], k, ((1,), (0,))) * scale).astype(BF)
        dk = dot(ds_low[:, :keys], q, ((0,), (0,))) * scale
        dv = dot(p_low[:, :keys], da, ((0,), (0,)))
        return dk, dv

    dk, dv = attend(
        sent, q_sl[sent], da_sl[sent], pick(sent, columns(k_ref)), pick(sent, columns(v_ref)), tile, None
    )
    dk_sl[sent, :, :HD] = dk.astype(BF)
    dk_sl[sent, :, HD:] = dv.astype(BF)
    for j in range(1, 4):
        at_copy(j, sent).start()

    def relay(i):
        for d in range(2):
            @pl.when(wide[1 - d][0])
            def _():
                w_copy(d, i).wait_recv()
        for d in range(2):
            @pl.when(high[d][0])
            def _():
                h_copy(d, 0, i).start()
                h_copy(d, 2, i).start()

    def fold_high(i):
        for d in range(2):
            @pl.when(high[1 - d][0])
            def _():
                bh_copy(d, i).wait_recv()
        for d in range(2):
            c = 2 * d
            side_out[i, d] = (
                acc[i, c] + back_in[i, 0, c].astype(F32) + back_in[i, 1, c].astype(F32)
            ).astype(BF)
        acc[i, 1] = acc[i, 1] + back_in[i, 0, 1].astype(F32) + back_in[i, 1, 1].astype(F32)
        for d in range(2):
            @pl.when(wide[d][0])
            def _():
                bw_copy(d, i).start()

    def fold_wide(i):
        for d in range(2):
            @pl.when(wide[1 - d][0])
            def _():
                bw_copy(d, i).wait_recv()
        dk_sl[i] = (
            acc[i, 1] + side_in[i, 0].astype(F32) + side_in[i, 1].astype(F32)
        ).astype(BF)

    def project(i):
        for j in range(1, 4):
            at_copy(j, i).wait_recv()
        part = dot(og_t[...], att[i].reshape(4 * tile, HD), ((1,), (0,)))
        for b in range(peers):
            dw_out[i, b] = part[b * block : (b + 1) * block].astype(BF)
        for b in range(1, peers):
            dw_copy(b, i).start()

    def window(i):
        def reach(c):
            return jnp.where(alone <= i, reach_ref[i + 1, c], reach_ref[i, c])

        tiles = lax.broadcasted_iota(jnp.int32, (1, 9 * tile), 1)
        bias = jnp.zeros((1, 9 * tile), F32)
        before = (jnp.where((ha > 0) & (reach(2) > 0), 1, 0), 1,
                  jnp.where((ha < n_ha - 1) & (reach(3) > 0), 1, 0))
        beside = (jnp.where((wa > 0) & (reach(4) > 0), 1, 0), 1,
                  jnp.where((wa < n_wa - 1) & (reach(5) > 0), 1, 0))
        for t in range(9):
            open_ = jnp.where(before[t // 3] * beside[t % 3] > 0, 0.0, OUTSIDE)
            inside = (tiles >= t * tile) & (tiles < (t + 1) * tile)
            bias = jnp.where(inside, open_, bias)
        return bias

    relay(0)
    relay(1)
    for j in range(1, 4):
        og_copy(j).wait_recv()
    og_g[0] = og_s[dp_lo * 2 + ha_lo]
    og_t[...] = og_g[...].reshape(4 * tile, quarter).T
    project(sent)

    def step(i, carry):
        pl.when(i + 2 < sent)(lambda: relay(i + 2))
        for d in range(2):
            @pl.when(high[1 - d][0])
            def _():
                for c in range(3):
                    h_copy(d, c, i).wait_recv()
        near = kv[i].reshape(9 * tile, 2 * HD)
        dk, dv = attend(
            i, q_sl[i], da_sl[i], near[:, :HD], near[:, HD:], 9 * tile, window(i)
        )
        for j in range(1, 4):
            at_copy(j, i).start()
        dk = dk.reshape(3, 3, tile, HD)
        dv = dv.reshape(3, 3, tile, HD)
        for d in range(2):
            back_out[i, d, :, :, :HD] = dk[2 * d].astype(BF)
            back_out[i, d, :, :, HD:] = dv[2 * d].astype(BF)

            @pl.when(high[d][0])
            def _():
                bh_copy(d, i).start()
        acc[i, :, :, :HD] = dk[1]
        acc[i, :, :, HD:] = dv[1]

        @pl.when(i >= 1)
        def _():
            project(i - 1)
            fold_high(i - 1)
        pl.when(i >= 2)(lambda: fold_wide(i - 2))
        return carry

    lax.fori_loop(0, sent, step, 0)
    project(sent - 1)
    fold_high(sent - 1)
    if sent > 1:
        fold_wide(sent - 2)

    def gather_w(i, carry):
        total = dw_out[i, my_peer].astype(F32)
        for b in range(1, peers):
            dw_copy(b, i).wait_recv()
            total = total + dw_in[i, b - 1].astype(F32)
        dw_sl[i] = total
        return carry

    lax.fori_loop(0, heads, gather_w, 0)
    fold_wide(sent - 1)
    def drain(i, carry):
        for d in range(2):
            @pl.when(wide[d][0])
            def _():
                w_copy(d, i).wait_send()
                bw_copy(d, i).wait_send()

            @pl.when(high[d][0])
            def _():
                for c in range(3):
                    h_copy(d, c, i).wait_send()
                bh_copy(d, i).wait_send()
        return carry

    lax.fori_loop(0, sent, drain, 0)

    def drain_w(i, carry):
        for j in range(1, 4):
            at_copy(j, i).wait_send()
        for b in range(1, peers):
            dw_copy(b, i).wait_send()
        return carry

    lax.fori_loop(0, heads, drain_w, 0)
    for j in range(1, 4):
        og_copy(j).wait_send()


def in_head_order(heads, reach_ref, dq_sl, dk_sl, dw_sl, gq_ref, gk_ref, gv_ref, gw_ref):
    alone = lone_head(heads, reach_ref)
    for n in range(heads):
        slot = jnp.where(alone == n, heads - 1, n - jnp.where(alone < n, 1, 0))
        at = slice(n * HD, (n + 1) * HD)
        gq_ref[:, at] = dq_sl[slot]
        gk_ref[:, at] = dk_sl[slot, :, :HD]
        gv_ref[:, at] = dk_sl[slot, :, HD:]
        gw_ref[:, at] = dw_sl[slot]


def shards(sizes, queries, key_tiles, value_tiles, out_grad, w_out, reaches):
    tile, width = queries.shape[4:]
    model = out_grad.shape[5]
    heads = width // HD
    sent = heads - 1
    devices = sizes[0] * sizes[1] * sizes[2]
    block = model // devices
    peers = devices // 4
    rows = [a.reshape(a.shape[-2:]) for a in (queries, key_tiles, value_tiles, out_grad)]
    sem = pltpu.SemaphoreType.DMA
    vmem = pl.BlockSpec(memory_space=pltpu.VMEM)
    smem = pl.BlockSpec(memory_space=pltpu.SMEM)
    grads = jax.ShapeDtypeStruct((tile, width), BF)
    slots = pl.pallas_call(
        functools.partial(kernel, sizes, heads),
        out_shape=(
            jax.ShapeDtypeStruct((heads, tile, HD), BF),
            jax.ShapeDtypeStruct((heads, tile, 2 * HD), BF),
            jax.ShapeDtypeStruct((heads, block, HD), F32),
        ),
        in_specs=[vmem] * 3 + [pl.BlockSpec(memory_space=pl.ANY)] * 2 + [smem],
        out_specs=(vmem,) * 3,
        scratch_shapes=[
            pltpu.VMEM((sent, 9, tile, 2 * HD), BF),
            pltpu.VMEM((heads, tile, HD), BF),
            pltpu.VMEM((heads, tile, HD), BF),
            pltpu.VMEM((4, tile, model // 4), BF),
            pltpu.VMEM((4, tile, model // 4), BF),
            pltpu.VMEM((model // 4, 4 * tile), BF),
            pltpu.VMEM((heads, 4, tile, HD), BF),
            pltpu.VMEM((tile, 9 * tile), F32),
            pltpu.VMEM((tile, 9 * tile), F32),
            pltpu.VMEM((tile, 9 * tile), BF),
            pltpu.VMEM((tile, 9 * tile), BF),
            pltpu.VMEM((sent, 2, 3, tile, 2 * HD), BF),
            pltpu.VMEM((sent, 2, 3, tile, 2 * HD), BF),
            pltpu.VMEM((sent, 2, tile, 2 * HD), BF),
            pltpu.VMEM((sent, 2, tile, 2 * HD), BF),
            pltpu.VMEM((sent, 3, tile, 2 * HD), F32),
            pltpu.VMEM((heads, peers, block, HD), BF),
            pltpu.VMEM((heads, peers - 1, block, HD), BF),
            pltpu.VMEM((tile, model), BF),
            pltpu.VMEM((model, width), BF),
            sem((2,)),
            sem((2, sent)), sem((2, sent)), sem((2, 3, sent)), sem((2, 3, sent)),
            sem((2, sent)), sem((2, sent)), sem((2, sent)), sem((2, sent)),
            sem((3,)), sem((3,)), sem((3, heads)), sem((3, heads)),
            sem((peers - 1, heads)), sem((peers - 1, heads)),
        ],
        compiler_params=pltpu.CompilerParams(
            collective_id=0, has_side_effects=True, vmem_limit_bytes=60 * 1024 * 1024
        ),
    )(*rows, w_out, reaches)
    out = pl.pallas_call(
        functools.partial(in_head_order, heads),
        out_shape=(grads, grads, grads, jax.ShapeDtypeStruct((block, width), F32)),
        in_specs=[smem] + [vmem] * 3,
        out_specs=(vmem,) * 4,
    )(reaches, *slots)
    return tuple(o.reshape(queries.shape) for o in out[:3]) + (out[3],)


def solution(mesh):
    tiles = P("dp", None, "ha", "wa", None, None)
    sizes = tuple(mesh.shape[a] for a in ("dp", "ha", "wa"))
    return jax.shard_map(
        functools.partial(shards, sizes),
        mesh=mesh,
        in_specs=(tiles, tiles, tiles, tiles, P(), P()),
        out_specs=(tiles, tiles, tiles, P(("dp", "ha", "wa"), None)),
        check_vma=False,
    )
```

```python
import functools
import math

import jax
import jax.numpy as jnp
from jax import lax
from jax.experimental import pallas as pl
from jax.experimental.pallas import tpu as pltpu
from jax.sharding import PartitionSpec as P

HD = 128
BF = jnp.bfloat16
F32 = jnp.float32
OUTSIDE = -1e30


def dot(a, b, dims):
    return lax.dot_general(a, b, (dims, ((), ())), preferred_element_type=F32)


def lone_head(heads, reach_ref):
    alone = jnp.int32(0)
    for n in reversed(range(heads)):
        reach = reach_ref[n, 2] + reach_ref[n, 3] + reach_ref[n, 4] + reach_ref[n, 5]
        alone = jnp.where(reach == 0, n, alone)
    return alone


def kernel(
    sizes, heads, q_ref, k_ref, v_ref, og_any, w_any, reach_ref, dq_sl, dk_sl, dw_sl,
    kv, q_sl, da_sl, og_s, og_g, og_t, att, s_ref, dp_ref, p_low, ds_low,
    back_out, back_in, side_out, side_in, acc, dw_out, dw_in, dz_out, dz_in, og_ref, w_ref, in_sem,
    w_send, w_recv, h_send, h_recv, bh_send, bh_recv, bw_send, bw_recv,
    og_send, og_recv, at_send, at_recv, dw_send, dw_recv, dz_send, dz_recv, x_send, x_recv,
):
    n_dp, n_ha, n_wa = sizes
    sent = heads - 1
    tile = q_ref.shape[0]
    model = og_ref.shape[1]
    quarter = model // 4
    block = dw_sl.shape[1]
    run = n_wa * block
    scale = 1.0 / math.sqrt(HD)
    dp, ha, wa = (lax.axis_index(a) for a in ("dp", "ha", "wa"))
    dp_hi, dp_lo = dp // 2, dp % 2
    ha_hi, ha_lo = ha // 2, ha % 2
    wide = ((wa > 0, (dp, ha, wa - 1)), (wa < n_wa - 1, (dp, ha, wa + 1)))
    high = ((ha > 0, (dp, ha - 1, wa)), (ha < n_ha - 1, (dp, ha + 1, wa)))
    group = []
    for j in range(1, 4):
        d_lo = (1 - dp_lo) if j // 2 else dp_lo
        h_lo = (1 - ha_lo) if j % 2 else ha_lo
        group.append((d_lo * 2 + h_lo, (dp_hi * 2 + d_lo, ha_hi * 2 + h_lo, wa)))
    runs = (n_dp // 2) * (n_ha // 2)
    peers = runs * n_wa
    my_run = dp_hi * (n_ha // 2) + ha_hi

    def run_at(step):
        r = lax.rem(my_run + step, runs)
        return r, ((r // (n_ha // 2)) * 2 + dp_lo, (r % (n_ha // 2)) * 2 + ha_lo, wa)

    def column_at(step):
        at = lax.rem(wa + step, n_wa)
        return at, (dp, ha, at)

    def remote(src, dst, s, r, device):
        return pltpu.make_async_remote_copy(
            src_ref=src, dst_ref=dst, send_sem=s, recv_sem=r, device_id=device,
            device_id_type=pl.DeviceIdType.MESH,
        )

    def w_copy(d, i):
        return remote(
            kv.at[i, 4], kv.at[i, 3 + 2 * (1 - d)], w_send.at[d, i], w_recv.at[d, i], wide[d][1]
        )

    def h_copy(d, c, i):
        return remote(
            kv.at[i, 3 + c], kv.at[i, 6 * (1 - d) + c], h_send.at[d, c, i], h_recv.at[d, c, i],
            high[d][1],
        )

    def bh_copy(d, i):
        return remote(
            back_out.at[i, d], back_in.at[i, d], bh_send.at[d, i], bh_recv.at[d, i], high[d][1]
        )

    def bw_copy(d, i):
        return remote(
            side_out.at[i, d], side_in.at[i, d], bw_send.at[d, i], bw_recv.at[d, i], wide[d][1]
        )

    def og_copy(j):
        member, device = group[j - 1]
        return remote(og_s.at[member], og_g.at[j], og_send.at[j - 1], og_recv.at[j - 1], device)

    def at_copy(j, i):
        return remote(
            att.at[i, 0], att.at[i, j], at_send.at[j - 1, i], at_recv.at[j - 1, i],
            group[j - 1][1],
        )

    def dw_copy(step, i):
        r, device = run_at(step)
        return remote(
            dw_out.at[i, r], dw_in.at[i, step - 1], dw_send.at[step - 1, i],
            dw_recv.at[step - 1, i], device,
        )

    def dz_copy(step, i):
        at, device = column_at(step)
        return remote(
            dz_out.at[i, at], dz_in.at[i, step - 1], dz_send.at[step - 1, i],
            dz_recv.at[step - 1, i], device,
        )

    def x_copy(d, e, i):
        return remote(
            kv.at[i, 6 * d + 1], kv.at[i, 6 * d + 2 * (1 - e)], x_send.at[d, e, i],
            x_recv.at[d, e, i], wide[e][1],
        )

    def crosses(d, i):
        return (i % 2 == 1) & (ha_lo == d)

    og_in = pltpu.make_async_copy(og_any, og_ref, in_sem.at[0])
    w_in = pltpu.make_async_copy(w_any, w_ref, in_sem.at[1])
    og_in.start()
    w_in.start()
    barrier = pltpu.get_barrier_semaphore()

    def greet(device):
        pl.semaphore_signal(
            barrier, inc=1, device_id=device, device_id_type=pl.DeviceIdType.MESH
        )

    for exists, device in wide + high:
        pl.when(exists)(functools.partial(greet, device))
    for _, device in group:
        greet(device)
    for step in range(1, runs):
        greet(run_at(step)[1])
    for step in range(1, n_wa):
        greet(column_at(step)[1])

    alone = lone_head(heads, reach_ref)

    def pick(i, read):
        if i < sent:
            return jnp.where(alone <= i, read(i + 1), read(i))
        value = read(0)
        for n in range(1, heads):
            value = jnp.where(alone == n, read(n), value)
        return value

    def columns(ref):
        return lambda n: ref[:, n * HD : (n + 1) * HD]

    for i in range(sent):
        kv[i, 4, :, :HD] = pick(i, columns(k_ref))
        kv[i, 4, :, HD:] = pick(i, columns(v_ref))
    for d in range(2):
        @pl.when(jnp.logical_not(wide[d][0]))
        def _():
            for i in range(sent):
                kv[i, 3 + 2 * d] = jnp.zeros((tile, 2 * HD), BF)
                side_in[i, 1 - d] = jnp.zeros((tile, 2 * HD), BF)
            for h in range(2):
                @pl.when(high[h][0] & (ha_lo == h))
                def _():
                    for i in range(1, sent, 2):
                        kv[i, 6 * h + 2 * d] = jnp.zeros((tile, 2 * HD), BF)

        @pl.when(jnp.logical_not(high[d][0]))
        def _():
            for i in range(sent):
                kv[i, 6 * d : 6 * d + 3] = jnp.zeros((3, tile, 2 * HD), BF)
                back_in[i, 1 - d] = jnp.zeros((3, tile, 2 * HD), BF)

    waits = 3 + runs - 1 + n_wa - 1
    for exists, _ in wide + high:
        waits = waits + jnp.where(exists, 1, 0)
    pl.semaphore_wait(barrier, waits)

    for i in range(sent):
        for d in range(2):
            @pl.when(wide[d][0])
            def _():
                w_copy(d, i).start()

            @pl.when(high[d][0])
            def _():
                h_copy(d, 1, i).start()
    og_in.wait()
    for m in range(4):
        for r in range(runs):
            first = (r // (n_ha // 2) * 2 + m // 2) * n_ha + (r % (n_ha // 2)) * 2 + m % 2
            og_s[m, :, r * run : (r + 1) * run] = og_ref[:, first * run : (first + 1) * run]
    for j in range(1, 4):
        og_copy(j).start()
    w_in.wait()

    grad_attn = dot(og_ref[...], w_ref[...], ((1,), (0,))).astype(BF)
    for i in range(heads):
        q_sl[i] = pick(i, columns(q_ref))
        da_sl[i] = pick(i, columns(grad_attn))

    def attend(i, q, da, k, v, keys, bias):
        def rows(c):
            return slice(c * 16, (c + 1) * 16)

        s_ref[:, :keys] = dot(q, k, ((1,), (1,)))
        dp_ref[:, :keys] = dot(da, v, ((1,), (1,)))
        for c in range(tile // 16):
            s = s_ref[rows(c), :keys] * scale
            if bias is not None:
                s = s + bias
            e = jnp.exp(s - jnp.max(s, axis=1, keepdims=True))
            p = e * (1.0 / jnp.sum(e, axis=1, keepdims=True))
            s_ref[rows(c), :keys] = p
            p_low[rows(c), :keys] = p.astype(BF)
        attended = dot(p_low[:, :keys], v, ((1,), (0,))).astype(BF)
        att[i, 0] = attended
        delta = jnp.sum(da.astype(F32) * attended.astype(F32), axis=1, keepdims=True)
        for c in range(tile // 16):
            ds = s_ref[rows(c), :keys] * (dp_ref[rows(c), :keys] - delta[rows(c)])
            ds_low[rows(c), :keys] = ds.astype(BF)
        dq_sl[i] = (dot(ds_low[:, :keys], k, ((1,), (0,))) * scale).astype(BF)
        dk = dot(ds_low[:, :keys], q, ((0,), (0,))) * scale
        dv = dot(p_low[:, :keys], da, ((0,), (0,)))
        return dk, dv

    dk, dv = attend(
        sent, q_sl[sent], da_sl[sent], pick(sent, columns(k_ref)), pick(sent, columns(v_ref)), tile, None
    )
    dk_sl[sent, :, :HD] = dk.astype(BF)
    dk_sl[sent, :, HD:] = dv.astype(BF)
    for j in range(1, 4):
        at_copy(j, sent).start()

    def relay(i):
        for d in range(2):
            @pl.when(wide[1 - d][0])
            def _():
                w_copy(d, i).wait_recv()
        for d in range(2):
            @pl.when(high[d][0] & jnp.logical_not(crosses(d, i)))
            def _():
                h_copy(d, 0, i).start()
                h_copy(d, 2, i).start()
        for d in range(2):
            @pl.when(high[d][0] & crosses(d, i))
            def _():
                h_copy(1 - d, 1, i).wait_recv()
                for e in range(2):
                    pl.when(wide[e][0])(lambda: x_copy(d, e, i).start())

    def fold_high(i):
        for d in range(2):
            @pl.when(high[1 - d][0])
            def _():
                bh_copy(d, i).wait_recv()
        for d in range(2):
            c = 2 * d
            side_out[i, d] = (
                acc[i, c] + back_in[i, 0, c].astype(F32) + back_in[i, 1, c].astype(F32)
            ).astype(BF)
        acc[i, 1] = acc[i, 1] + back_in[i, 0, 1].astype(F32) + back_in[i, 1, 1].astype(F32)
        for d in range(2):
            @pl.when(wide[d][0])
            def _():
                bw_copy(d, i).start()

    def fold_wide(i):
        for d in range(2):
            @pl.when(wide[1 - d][0])
            def _():
                bw_copy(d, i).wait_recv()
        dk_sl[i] = (
            acc[i, 1] + side_in[i, 0].astype(F32) + side_in[i, 1].astype(F32)
        ).astype(BF)

    def project(i):
        for j in range(1, 4):
            at_copy(j, i).wait_recv()
        part = dot(og_t[...], att[i].reshape(4 * tile, HD), ((1,), (0,)))
        for b in range(peers):
            rows = part[b * block : (b + 1) * block]
            dw_out[i, b // n_wa, b % n_wa] = rows.astype(BF)
        for b in range(1, runs):
            dw_copy(b, i).start()

    def pass_on(i):
        total = dw_out[i, my_run].astype(F32)
        for b in range(1, runs):
            dw_copy(b, i).wait_recv()
            total = total + dw_in[i, b - 1].astype(F32)
        dz_out[i] = total.astype(BF)
        for b in range(1, n_wa):
            dz_copy(b, i).start()

    def window(i):
        def reach(c):
            return jnp.where(alone <= i, reach_ref[i + 1, c], reach_ref[i, c])

        tiles = lax.broadcasted_iota(jnp.int32, (1, 9 * tile), 1)
        bias = jnp.zeros((1, 9 * tile), F32)
        before = (jnp.where((ha > 0) & (reach(2) > 0), 1, 0), 1,
                  jnp.where((ha < n_ha - 1) & (reach(3) > 0), 1, 0))
        beside = (jnp.where((wa > 0) & (reach(4) > 0), 1, 0), 1,
                  jnp.where((wa < n_wa - 1) & (reach(5) > 0), 1, 0))
        for t in range(9):
            open_ = jnp.where(before[t // 3] * beside[t % 3] > 0, 0.0, OUTSIDE)
            inside = (tiles >= t * tile) & (tiles < (t + 1) * tile)
            bias = jnp.where(inside, open_, bias)
        return bias

    relay(0)
    relay(1)
    for j in range(1, 4):
        og_copy(j).wait_recv()
    og_g[0] = og_s[dp_lo * 2 + ha_lo]
    og_t[...] = og_g[...].reshape(4 * tile, quarter).T
    project(sent)

    def step(i, carry):
        pl.when(i + 2 < sent)(lambda: relay(i + 2))
        for d in range(2):
            @pl.when(high[1 - d][0] & jnp.logical_not(crosses(1 - d, i)))
            def _():
                for c in range(3):
                    h_copy(d, c, i).wait_recv()

            @pl.when(high[1 - d][0] & crosses(1 - d, i))
            def _():
                for e in range(2):
                    pl.when(wide[1 - e][0])(lambda: x_copy(1 - d, e, i).wait_recv())
        near = kv[i].reshape(9 * tile, 2 * HD)
        dk, dv = attend(
            i, q_sl[i], da_sl[i], near[:, :HD], near[:, HD:], 9 * tile, window(i)
        )
        for j in range(1, 4):
            at_copy(j, i).start()
        dk = dk.reshape(3, 3, tile, HD)
        dv = dv.reshape(3, 3, tile, HD)
        for d in range(2):
            back_out[i, d, :, :, :HD] = dk[2 * d].astype(BF)
            back_out[i, d, :, :, HD:] = dv[2 * d].astype(BF)

            @pl.when(high[d][0])
            def _():
                bh_copy(d, i).start()
        acc[i, :, :, :HD] = dk[1]
        acc[i, :, :, HD:] = dv[1]

        @pl.when(i >= 1)
        def _():
            project(i - 1)
            fold_high(i - 1)

        pl.when(i == 0)(lambda: pass_on(sent))

        @pl.when(i >= 2)
        def _():
            pass_on(i - 2)
            fold_wide(i - 2)

        return carry

    lax.fori_loop(0, sent, step, 0)
    project(sent - 1)
    fold_high(sent - 1)
    pass_on(sent - 2)
    fold_wide(sent - 2)
    pass_on(sent - 1)

    def gather_w(i, carry):
        total = dz_out[i, wa].astype(F32)
        for b in range(1, n_wa):
            dz_copy(b, i).wait_recv()
            total = total + dz_in[i, b - 1].astype(F32)
        dw_sl[i] = total
        return carry

    lax.fori_loop(0, heads, gather_w, 0)
    fold_wide(sent - 1)
    def drain(i, carry):
        for d in range(2):
            @pl.when(wide[d][0])
            def _():
                w_copy(d, i).wait_send()
                bw_copy(d, i).wait_send()

            @pl.when(high[d][0])
            def _():
                h_copy(d, 1, i).wait_send()
                bh_copy(d, i).wait_send()

            @pl.when(high[d][0] & jnp.logical_not(crosses(d, i)))
            def _():
                h_copy(d, 0, i).wait_send()
                h_copy(d, 2, i).wait_send()

            @pl.when(high[d][0] & crosses(d, i))
            def _():
                for e in range(2):
                    pl.when(wide[e][0])(lambda: x_copy(d, e, i).wait_send())
        return carry

    lax.fori_loop(0, sent, drain, 0)

    def drain_w(i, carry):
        for j in range(1, 4):
            at_copy(j, i).wait_send()
        for b in range(1, runs):
            dw_copy(b, i).wait_send()
        for b in range(1, n_wa):
            dz_copy(b, i).wait_send()
        return carry

    lax.fori_loop(0, heads, drain_w, 0)
    for j in range(1, 4):
        og_copy(j).wait_send()


def in_head_order(heads, reach_ref, dq_sl, dk_sl, dw_sl, gq_ref, gk_ref, gv_ref, gw_ref):
    alone = lone_head(heads, reach_ref)
    for n in range(heads):
        slot = jnp.where(alone == n, heads - 1, n - jnp.where(alone < n, 1, 0))
        at = slice(n * HD, (n + 1) * HD)
        gq_ref[:, at] = dq_sl[slot]
        gk_ref[:, at] = dk_sl[slot, :, :HD]
        gv_ref[:, at] = dk_sl[slot, :, HD:]
        gw_ref[:, at] = dw_sl[slot]


def shards(sizes, queries, key_tiles, value_tiles, out_grad, w_out, reaches):
    tile, width = queries.shape[4:]
    model = out_grad.shape[5]
    heads = width // HD
    sent = heads - 1
    devices = sizes[0] * sizes[1] * sizes[2]
    block = model // devices
    columns = sizes[2]
    runs = devices // 4 // columns
    rows = [a.reshape(a.shape[-2:]) for a in (queries, key_tiles, value_tiles, out_grad)]
    sem = pltpu.SemaphoreType.DMA
    vmem = pl.BlockSpec(memory_space=pltpu.VMEM)
    smem = pl.BlockSpec(memory_space=pltpu.SMEM)
    grads = jax.ShapeDtypeStruct((tile, width), BF)
    slots = pl.pallas_call(
        functools.partial(kernel, sizes, heads),
        out_shape=(
            jax.ShapeDtypeStruct((heads, tile, HD), BF),
            jax.ShapeDtypeStruct((heads, tile, 2 * HD), BF),
            jax.ShapeDtypeStruct((heads, block, HD), F32),
        ),
        in_specs=[vmem] * 3 + [pl.BlockSpec(memory_space=pl.ANY)] * 2 + [smem],
        out_specs=(vmem,) * 3,
        scratch_shapes=[
            pltpu.VMEM((sent, 9, tile, 2 * HD), BF),
            pltpu.VMEM((heads, tile, HD), BF),
            pltpu.VMEM((heads, tile, HD), BF),
            pltpu.VMEM((4, tile, model // 4), BF),
            pltpu.VMEM((4, tile, model // 4), BF),
            pltpu.VMEM((model // 4, 4 * tile), BF),
            pltpu.VMEM((heads, 4, tile, HD), BF),
            pltpu.VMEM((tile, 9 * tile), F32),
            pltpu.VMEM((tile, 9 * tile), F32),
            pltpu.VMEM((tile, 9 * tile), BF),
            pltpu.VMEM((tile, 9 * tile), BF),
            pltpu.VMEM((sent, 2, 3, tile, 2 * HD), BF),
            pltpu.VMEM((sent, 2, 3, tile, 2 * HD), BF),
            pltpu.VMEM((sent, 2, tile, 2 * HD), BF),
            pltpu.VMEM((sent, 2, tile, 2 * HD), BF),
            pltpu.VMEM((sent, 3, tile, 2 * HD), F32),
            pltpu.VMEM((heads, runs, columns, block, HD), BF),
            pltpu.VMEM((heads, runs - 1, columns, block, HD), BF),
            pltpu.VMEM((heads, columns, block, HD), BF),
            pltpu.VMEM((heads, columns - 1, block, HD), BF),
            pltpu.VMEM((tile, model), BF),
            pltpu.VMEM((model, width), BF),
            sem((2,)),
            sem((2, sent)), sem((2, sent)), sem((2, 3, sent)), sem((2, 3, sent)),
            sem((2, sent)), sem((2, sent)), sem((2, sent)), sem((2, sent)),
            sem((3,)), sem((3,)), sem((3, heads)), sem((3, heads)),
            sem((runs - 1, heads)), sem((runs - 1, heads)),
            sem((columns - 1, heads)), sem((columns - 1, heads)),
            sem((2, 2, sent)), sem((2, 2, sent)),
        ],
        compiler_params=pltpu.CompilerParams(
            collective_id=0, has_side_effects=True, vmem_limit_bytes=60 * 1024 * 1024
        ),
    )(*rows, w_out, reaches)
    out = pl.pallas_call(
        functools.partial(in_head_order, heads),
        out_shape=(grads, grads, grads, jax.ShapeDtypeStruct((block, width), F32)),
        in_specs=[smem] + [vmem] * 3,
        out_specs=(vmem,) * 4,
    )(reaches, *slots)
    return tuple(o.reshape(queries.shape) for o in out[:3]) + (out[3],)


def solution(mesh):
    tiles = P("dp", None, "ha", "wa", None, None)
    sizes = tuple(mesh.shape[a] for a in ("dp", "ha", "wa"))
    return jax.shard_map(
        functools.partial(shards, sizes),
        mesh=mesh,
        in_specs=(tiles, tiles, tiles, tiles, P(), P()),
        out_specs=(tiles, tiles, tiles, P(("dp", "ha", "wa"), None)),
        check_vma=False,
    )
```
